32 devices in a mesh: row: 2 (over core), col: 16 (over z, y, x).
Axes of the slice: x: 2, y: 2, z: 4, core: 2. Of those that a mesh axis runs over, the one named last changes fastest.
Arguments:
- movie: bfloat16 [128, 1024, 256], P('row', 'col'), may hold values from 0 to 1.5
- footprints: float32 [2, 16, 12, 4096], P('row', 'col'), may hold values from 0.05 to 1
- anchors: int32 [2, 16, 12, 2], P('row', 'col'), may hold values from 0 to 63, as said below
- groups: int32 [2, 16, 12], P('row', 'col'), may hold values from 0 to 3, as said below
- counts: int32 [2, 16], P('row', 'col'), may hold values from 1 to 12, as said below
- temporal: float32 [2, 16, 12, 256], P('row', 'col'), may hold values from 0.2 to 2
- back_spatial: bfloat16 [2, 128, 1024], P(None, 'row', 'col'), may hold values from 0 to 0.5
- back_temporal: float32 [2, 256], replicated, may hold values from 0.5 to 1
- window: int32 [2], replicated, may hold values from 0 to 256, as said below
Outputs:
- new_footprints: float32 [2, 16, 12, 4096], P('row', 'col')
- new_traces: float32 [2, 16, 12, 256], P('row', 'col')
The draws below stay inside these ranges and needn't reach their ends.
Inputs may be any that keep to these rules, and one draw needn't show every extreme that they name: `anchors`: a block's anchor lies in its tile; on the last tile row the row offset is at most 0, on the last tile column the column offset at most 0. `counts`: slots below the count are live, the others are ignored; some tile has 12 live slots. `groups`: every tile has exactly 3 slots, live or not, in each group. window[0] is at most 64 and window[1] at least 192.
All inputs are finite; a program needn't handle non-finite values.
Results may differ from the reference program's by a relative error of at most 0.00084.
Values may be sent and summed in bfloat16 or wider, within the bound.
No kernel may reach another device: no remote copies, remote signals or barrier semaphores. Data moves between devices by JAX's collectives and lax.ppermute only.
A program may use at most 64 MiB of HBM per device.

```python
import math
from functools import partial
import jax
import jax.numpy as jnp
from jax import lax

TH = 64
TW = 64
FRAMES = 256
FP = 64
MAXN = 12
GROUPS = 4
HEIGHT = 128
WIDTH = 1024
N_ROW = 2
N_COL = 16


def draw_anchors(key, part):
    grid_rows = HEIGHT // TH
    grid_cols = WIDTH // TW
    row_ids = jnp.arange(grid_rows, dtype=jnp.int32)[:, None, None]
    col_ids = jnp.arange(grid_cols, dtype=jnp.int32)[None, :, None]
    high_rows = jnp.broadcast_to(jnp.where(row_ids == grid_rows - 1, TH - FP + 1, TH), (grid_rows, grid_cols, MAXN))
    high_cols = jnp.broadcast_to(jnp.where(col_ids == grid_cols - 1, TW - FP + 1, TW), (grid_rows, grid_cols, MAXN))
    downs = jax.random.randint(jax.random.fold_in(key, 11), (grid_rows, grid_cols, MAXN), 0, high_rows)
    rights = jax.random.randint(jax.random.fold_in(key, 12), (grid_rows, grid_cols, MAXN), 0, high_cols)
    return jnp.stack([downs, rights], axis=-1).astype(jnp.int32)


def draw_groups(key, part):
    grid_rows = HEIGHT // TH
    grid_cols = WIDTH // TW
    slot_ids = jnp.arange(MAXN, dtype=jnp.int32)[None, None, :]
    scores = jax.random.randint(jax.random.fold_in(key, 41), (grid_rows, grid_cols, MAXN), 0, 1 << 20) * MAXN + slot_ids
    ordering = jnp.argsort(scores, axis=-1, stable=True)
    ranking = jnp.argsort(ordering, axis=-1, stable=True)
    return (ranking % GROUPS).astype(jnp.int32)


def draw_counts(key, part):
    grid_rows = HEIGHT // TH
    grid_cols = WIDTH // TW
    layout = (grid_rows, grid_cols)
    base = jax.random.randint(jax.random.fold_in(key, 21), layout, 1, min(MAXN // 2 + 3, MAXN + 1))
    crowded = jax.random.randint(jax.random.fold_in(key, 22), layout, 0, 8) == 0
    marked_at = jax.random.randint(jax.random.fold_in(key, 23), (), 0, grid_rows * grid_cols)
    marked = jnp.arange(grid_rows * grid_cols, dtype=jnp.int32).reshape(layout) == marked_at
    return jnp.where(crowded | marked, MAXN, base).astype(jnp.int32)


def draw_window(key, part):
    first = jax.random.randint(jax.random.fold_in(key, 31), (), 0, FRAMES // 4 + 1)
    last = jax.random.randint(jax.random.fold_in(key, 32), (), 3 * FRAMES // 4, FRAMES + 1)
    return jnp.stack([first, last]).astype(jnp.int32)


def block_scale(rng, shape, pieces, least, high):
    def one(axis_at, blocks):
        steps = jax.random.uniform(jax.random.fold_in(jax.random.fold_in(rng, 6), axis_at), (blocks,), jnp.float32, least / len(pieces), high / len(pieces))
        return jnp.repeat(jnp.exp(steps), shape[axis_at] // blocks).reshape((-1,) + (1,) * (len(shape) - axis_at - 1))

    loudness = one(*pieces[0])
    for cut in pieces[1:]:
        loudness = loudness * one(*cut)
    return loudness


def setup_inputs(seed: int = 0) -> dict:
    arg_keys = jax.random.split(jax.random.key(seed), 10)
    return {
        "movie": jnp.clip(1.5 * jax.random.uniform(arg_keys[0], (HEIGHT, WIDTH, FRAMES), jnp.float32) ** block_scale(arg_keys[0], (HEIGHT, WIDTH, FRAMES), ((0, 2), (1, 16)), -0.2, 0.2), 0.0, 1.5).astype(jnp.bfloat16),
        "footprints": jnp.clip(jnp.exp(math.log(1.0) - 2.9957323 * jax.random.uniform(arg_keys[1], (N_ROW, N_COL, MAXN, FP * FP), jnp.float32) ** block_scale(arg_keys[1], (N_ROW, N_COL, MAXN, FP * FP), ((0, 2), (1, 16)), -0.2, 0.2)), 0.05, 1.0),
        "anchors": draw_anchors(jax.random.fold_in(arg_keys[9], 71), 0),
        "groups": draw_groups(jax.random.fold_in(arg_keys[9], 71), 0),
        "counts": draw_counts(jax.random.fold_in(arg_keys[9], 71), 0),
        "temporal": jnp.clip(jnp.exp(math.log(2.0) - 2.3025851 * jax.random.uniform(arg_keys[5], (N_ROW, N_COL, MAXN, FRAMES), jnp.float32) ** block_scale(arg_keys[5], (N_ROW, N_COL, MAXN, FRAMES), ((0, 2), (1, 16)), -0.2, 0.2)), 0.2, 2.0),
        "back_spatial": jnp.clip(0.5 * jax.random.uniform(arg_keys[6], (2, HEIGHT, WIDTH), jnp.float32) ** block_scale(arg_keys[6], (2, HEIGHT, WIDTH), ((1, 2), (2, 16)), -0.2, 0.2), 0.0, 0.5).astype(jnp.bfloat16),
        "back_temporal": jnp.clip(jax.random.uniform(arg_keys[7], (2, FRAMES), jnp.float32, 0.5, 1.0), 0.5, 1.0),
        "window": draw_window(jax.random.fold_in(arg_keys[9], 71), 0),
    }


exact_mode = lax.Precision.HIGHEST


def grid_pad(values):
    widths = [(1, 1), (1, 1)] + [(0, 0)] * (values.ndim - 2)
    return jnp.pad(values, widths)


def near_block(padded, row_at, col_at):
    nought = jnp.zeros((), jnp.int32)
    starts = (row_at, col_at) + (nought,) * (padded.ndim - 2)
    return lax.dynamic_slice(padded, starts, (3, 3) + padded.shape[2:])


def place_block(block, top_row, left_col, height, width):
    sheet = jnp.zeros((height + 2 * FP, width + 2 * FP), jnp.float32)
    within = ((top_row >= -FP) & (top_row <= height) & (left_col >= -FP) & (left_col <= width)).astype(jnp.float32)
    at_row = jnp.clip(top_row + FP, 0, height + FP).astype(jnp.int32)
    at_col = jnp.clip(left_col + FP, 0, width + FP).astype(jnp.int32)
    sheet = lax.dynamic_update_slice(sheet, block * within, (at_row, at_col))
    return sheet[FP:FP + height, FP:FP + width]


def lift_block(values, top_row, left_col, height, width):
    padded = jnp.pad(values, FP)
    within = ((top_row >= -FP) & (left_col >= -FP)).astype(jnp.float32)
    at_row = jnp.clip(top_row + FP, 0, height + FP).astype(jnp.int32)
    at_col = jnp.clip(left_col + FP, 0, width + FP).astype(jnp.int32)
    return lax.dynamic_slice(padded, (at_row, at_col), (FP, FP)) * within


def reference(movie, footprints, anchors, groups, counts, temporal, back_spatial, back_temporal, window):
    living = (jnp.arange(MAXN, dtype=jnp.int32)[None, None, :] < counts[:, :, None]).astype(jnp.float32)
    shapes = footprints * living[..., None]
    shape_grid = grid_pad(shapes)
    anchor_grid = grid_pad(anchors)
    group_grid = grid_pad(groups)
    living_grid = grid_pad(living)
    trace_grid = grid_pad(temporal)
    movie_padded = jnp.pad(movie, ((0, FP), (0, FP), (0, 0)))
    back_padded = jnp.pad(back_spatial, ((0, 0), (0, FP), (0, FP)))
    moments = jnp.arange(FRAMES, dtype=jnp.int32)
    inside = ((moments >= window[0]) & (moments < window[1])).astype(jnp.float32)
    tile_step = jnp.arange(3, dtype=jnp.int32) - 1
    nought = jnp.zeros((), jnp.int32)

    def tile_work(index):
        row_at = (index // N_COL).astype(jnp.int32)
        col_at = (index % N_COL).astype(jnp.int32)
        near_shape = near_block(shape_grid, row_at, col_at).reshape(9 * MAXN, FP, FP)
        near_anchor = near_block(anchor_grid, row_at, col_at)
        top_rows = (near_anchor[..., 0] + tile_step[:, None, None] * TH).reshape(9 * MAXN)
        left_cols = (near_anchor[..., 1] + tile_step[None, :, None] * TW).reshape(9 * MAXN)
        near_group = near_block(group_grid, row_at, col_at)[:2, :2].reshape(4 * MAXN)
        near_living = near_block(living_grid, row_at, col_at)[:2, :2].reshape(4 * MAXN)
        canvas = jax.vmap(partial(place_block, height=TH + FP, width=TW + FP))(near_shape, top_rows, left_cols)
        flattened = canvas.reshape(9 * MAXN, (TH + FP) * (TW + FP))
        owned = flattened[4 * MAXN:5 * MAXN]
        coupling = jnp.dot(owned, flattened.T, precision=exact_mode)
        movie_ext = lax.dynamic_slice(movie_padded, (row_at * TH, col_at * TW, nought), (TH + FP, TW + FP, FRAMES))
        movie_ext = movie_ext.astype(jnp.float32).reshape((TH + FP) * (TW + FP), FRAMES)
        back_ext = lax.dynamic_slice(back_padded, (nought, row_at * TH, col_at * TW), (2, TH + FP, TW + FP))
        back_ext = back_ext.astype(jnp.float32).reshape(2, (TH + FP) * (TW + FP))
        rounded = lax.optimization_barrier(owned.astype(jnp.bfloat16)).astype(jnp.float32)
        loadings = jnp.dot(owned, back_ext.T, precision=exact_mode)
        drives = jnp.dot(rounded, movie_ext, precision=exact_mode) - jnp.dot(loadings, back_temporal, precision=exact_mode)

        tile_canvas = canvas.reshape(3, 3, MAXN, TH + FP, TW + FP)[:2, :2, :, :TH, :TW].reshape(4 * MAXN, TH * TW)
        tile_top = top_rows.reshape(3, 3, MAXN)[:2, :2].reshape(4 * MAXN)
        tile_left = left_cols.reshape(3, 3, MAXN)[:2, :2].reshape(4 * MAXN)
        ones = jnp.ones((4 * MAXN, FP, FP), jnp.float32)
        cover = jax.vmap(partial(place_block, height=TH, width=TW))(ones, tile_top, tile_left).reshape(4 * MAXN, TH * TW)
        cover = cover * near_living[:, None]
        tile_traces = near_block(trace_grid, row_at, col_at)[:2, :2].reshape(4 * MAXN, FRAMES)
        weighted = tile_traces * inside[None, :]
        intersection_time = jnp.dot(weighted, weighted.T, precision=exact_mode)
        masses = jnp.diagonal(intersection_time)
        safe_mass = jnp.where(near_living > 0, masses, 1.0)
        tile_movie = lax.dynamic_slice(movie, (row_at * TH, col_at * TW, nought), (TH, TW, FRAMES))
        tile_movie = tile_movie.astype(jnp.float32).reshape(TH * TW, FRAMES)
        tile_back = lax.dynamic_slice(back_spatial, (nought, row_at * TH, col_at * TW), (2, TH, TW))
        tile_back = tile_back.astype(jnp.float32).reshape(2, TH * TW)
        trace_round = lax.optimization_barrier(weighted.astype(jnp.bfloat16)).astype(jnp.float32)
        back_loads = jnp.dot(weighted, back_temporal.T, precision=exact_mode)
        target = jnp.dot(trace_round, tile_movie.T, precision=exact_mode) - jnp.dot(back_loads, tile_back, precision=exact_mode)
        values = tile_canvas
        for step in range(GROUPS):
            coupled = jnp.dot(intersection_time, values, precision=exact_mode)
            chosen = cover * (near_group == step).astype(jnp.float32)[:, None]
            updated = jnp.maximum(values + (target - coupled) / safe_mass[:, None], 0.0)
            values = jnp.where(chosen > 0, updated, values)
        blocks = jax.vmap(partial(lift_block, height=TH, width=TW))(values.reshape(4 * MAXN, TH, TW), tile_top, tile_left)
        return drives, coupling, blocks.reshape(2, 2, MAXN, FP * FP)

    drives, couplings, blocks = lax.map(tile_work, jnp.arange(N_ROW * N_COL, dtype=jnp.int32))
    drives = drives.reshape(N_ROW, N_COL, MAXN, FRAMES)
    couplings = couplings.reshape(N_ROW, N_COL, MAXN, 9 * MAXN)
    blocks = blocks.reshape(N_ROW, N_COL, 2, 2, MAXN, FP * FP)
    padded = jnp.pad(blocks, ((0, 1), (0, 1), (0, 0), (0, 0), (0, 0), (0, 0)))
    new_shapes = padded[:-1, :-1, 1, 1] + padded[:-1, 1:, 1, 0] + padded[1:, :-1, 0, 1] + padded[1:, 1:, 0, 0]
    self_weight = jnp.diagonal(couplings[..., 4 * MAXN:5 * MAXN], axis1=2, axis2=3)
    safe_self = jnp.where(living > 0, self_weight, 1.0)
    traces = temporal
    for step in range(GROUPS):
        grid = grid_pad(traces)
        nearby = jnp.stack([grid[down_at:down_at + N_ROW, right_at:right_at + N_COL] for down_at in range(3) for right_at in range(3)], axis=2)
        nearby = nearby.reshape(N_ROW, N_COL, 9 * MAXN, FRAMES)
        coupled = jnp.einsum('rcnm,rcmt->rcnt', couplings, nearby, precision=exact_mode)
        chosen = living * (groups == step).astype(jnp.float32)
        updated = jnp.maximum(traces + (drives - coupled) / safe_self[..., None], 0.0)
        traces = jnp.where(chosen[..., None] > 0, updated, traces)
    return new_shapes, traces
```

```python
import functools
import math

import jax
import jax.numpy as jnp
from jax import lax
from jax.experimental import pallas as pl
from jax.experimental.pallas import tpu as pltpu
from jax.sharding import PartitionSpec as P

GROUPS = 4
LANES = 128
SUBLANES = 8
TRANS_B = (((1,), (1,)), ((), ()))


def lane_iota(shape):
    return lax.broadcasted_iota(jnp.int32, shape, 1)


def sub_iota(shape):
    return lax.broadcasted_iota(jnp.int32, shape, 0)


def rolled(strips, down, right, side):
    rows = strips[0].shape[0]
    lane = lane_iota((rows, LANES))
    odd = (down % 2) == 1
    source = (lane // side) * side + (lane - right + side) % side
    source = jnp.where(odd, (source + side) % LANES, source)
    moved = [jnp.take_along_axis(strip, source, axis=1, mode="promise_in_bounds") for strip in strips]
    carry = odd & (lane < side)
    count = len(strips)
    moved = [jnp.where(carry, moved[at - 1], moved[at]) for at in range(count)]
    jump = down // 2
    bit = 1
    while bit < count:
        take = (jump // bit) % 2 == 1
        moved = [jnp.where(take, moved[(at - bit) % count], moved[at]) for at in range(count)]
        bit *= 2
    return moved


def half_swap(values):
    return pltpu.roll(values, SUBLANES // 2, axis=0)


def column_of(row, size):
    at = sub_iota((size, size)) == lane_iota((size, size))
    return jnp.sum(jnp.where(at, jnp.broadcast_to(row, (size, size)), 0), axis=1, keepdims=True)


class Sizes:
    def __init__(self, pixels, frames):
        self.pixels, self.frames = pixels, frames
        self.rest = pixels
        self.trace = pixels + pixels // 2
        self.trace_rest = self.trace + frames
        self.info = self.trace_rest + frames // 2
        self.packed = self.info + LANES


def fold_rest(rest):
    half = rest.shape[1] // 2
    full = jnp.concatenate([rest, jnp.zeros_like(rest)], axis=0)
    return jnp.where(sub_iota((SUBLANES, half)) < 4, full[:, :half], half_swap(full[:, half:]))


def pack_kernel(sizes, side, footprint_ref, anchor_ref, group_ref, count_ref, trace_ref, out_ref):
    slots = anchor_ref.shape[1]
    count = sizes.pixels // LANES
    down, right = column_of(anchor_ref[0:1, :], slots), column_of(anchor_ref[1:2, :], slots)
    group = column_of(group_ref[...], slots)
    alive = sub_iota((slots, 1)) < count_ref[0, 0]
    strips = [jnp.where(alive, footprint_ref[pl.ds(at, slots, stride=count), :], 0.0) for at in range(count)]
    strips = rolled(strips, down, right, side)
    for at, strip in enumerate(strips):
        out_ref[:, at * LANES : (at + 1) * LANES] = strip[:SUBLANES]
    for at in range(count // 2):
        pair = jnp.concatenate([strips[at][SUBLANES:], strips[at + count // 2][SUBLANES:]], axis=0)
        out_ref[:, sizes.rest + at * LANES : sizes.rest + (at + 1) * LANES] = pair
    count = sizes.frames // LANES
    strips = [trace_ref[pl.ds(at, slots, stride=count), :] for at in range(count)]
    for at, strip in enumerate(strips):
        out_ref[:, sizes.trace + at * LANES : sizes.trace + (at + 1) * LANES] = strip[:SUBLANES]
    for at in range(count // 2):
        pair = jnp.concatenate([strips[at][SUBLANES:], strips[at + count // 2][SUBLANES:]], axis=0)
        out_ref[:, sizes.trace_rest + at * LANES : sizes.trace_rest + (at + 1) * LANES] = pair
    lane = lane_iota((slots, LANES))
    info = jnp.where(lane == 0, down, jnp.where(lane == 1, right, jnp.where(lane == 2, group, alive.astype(jnp.int32))))
    info = jnp.where(lane < 4, info, 0).astype(jnp.float32)
    rest = jnp.concatenate([info[SUBLANES:], jnp.zeros((SUBLANES * 2 - slots, LANES), jnp.float32)], axis=0)
    out_ref[:, sizes.info : sizes.info + LANES] = info[:SUBLANES] + pltpu.roll(rest, 4, axis=1)


def movie_kernel(after_ref, movie_ref, out_ref, sem):
    copy = pltpu.make_async_copy(movie_ref, out_ref, sem)
    copy.start()
    copy.wait()


def gather_rows(tops, rests):
    rows = list(tops)
    low = sub_iota(rests[0].shape) < 4
    for one, two in ((0, 1), (2, 3)):
        first = jnp.where(low, rests[one], half_swap(rests[two]))
        second = jnp.where(low, half_swap(rests[one]), rests[two])
        rows.append(jnp.concatenate([first, second], axis=1))
    return jnp.concatenate(rows, axis=0)


def tile_labels(sizes, tiles):
    infos = [tile[:, sizes.info :] for tile in tiles]
    turned = [pltpu.roll(info, LANES - 4, axis=1) for info in infos]
    low = sub_iota((SUBLANES, LANES)) < 4
    labels = jnp.concatenate(
        infos
        + [jnp.where(low, turned[0], half_swap(turned[1])), jnp.where(low, turned[2], half_swap(turned[3]))],
        axis=0,
    )
    down, right = labels[:, 0:1].astype(jnp.int32), labels[:, 1:2].astype(jnp.int32)
    group = jnp.where(labels[:, 3:4] > 0, labels[:, 2:3].astype(jnp.int32), -1)
    row = sub_iota(group.shape)
    block = jnp.where(row < 32, row // 8, (row - 32) // 4)
    return down, right, group, block >= 2, (block % 2) == 1


def tile_traces(sizes, tiles):
    return gather_rows(
        [tile[:, sizes.trace : sizes.trace + sizes.frames] for tile in tiles],
        [tile[:, sizes.trace_rest : sizes.trace_rest + sizes.frames // 2] for tile in tiles],
    )


def share_kernel(
    sizes, side, devices, own_ref, west_ref, north_ref, corner_ref, movie_ref, back_ref, back_trace_ref,
    value_ref, code_ref, split_ref, *outs,
):
    tiles = (own_ref, west_ref, north_ref, corner_ref)
    count = split_ref.shape[0] // 2 - 8
    pixels, frames = sizes.pixels, sizes.frames
    part = 512
    down, right, group, from_north, from_west = tile_labels(sizes, tiles)
    lane = lane_iota((count, part))
    for at in range(0, pixels, part):
        half = pixels // 2
        tops = [tile[:, at : at + part] for tile in tiles]
        where_rest = sizes.rest + at % half
        rests = [tile[:, where_rest : where_rest + part] for tile in tiles]
        sub_low = sub_iota((SUBLANES, part)) < 4
        pairs = []
        for one, two in ((0, 1), (2, 3)):
            if at < half:
                pairs.append(jnp.where(sub_low, rests[one], half_swap(rests[two])))
            else:
                pairs.append(jnp.where(sub_low, half_swap(rests[one]), rests[two]))
        raw = jnp.concatenate(tops + pairs, axis=0)
        spot = lane + at
        above, before = (spot // side) < down, (spot % side) < right
        covered = (above == from_north) & (before == from_west)
        value = jnp.where(covered, raw, 0.0)
        value_ref[:, at : at + part] = value
        code_ref[:, at : at + part] = jnp.where(covered, group, -1)
        high = value.astype(jnp.bfloat16)
        split_ref[0:count, at : at + part] = high
        split_ref[count : 2 * count, at : at + part] = (value - high.astype(jnp.float32)).astype(jnp.bfloat16)
    split_ref[2 * count : 2 * count + 16, :] = back_ref[...]
    share = jnp.dot(split_ref[0:count, :], movie_ref[...], preferred_element_type=jnp.float32)
    product = lax.dot_general(
        split_ref[0 : 2 * count, :], split_ref[...], TRANS_B, preferred_element_type=jnp.float32
    )
    product = product[:count] + product[count:]
    gram = product[:, :count] + product[:, count : 2 * count]
    for at in range(2):
        share = share - product[:, 2 * count + at : 2 * count + at + 1] * back_trace_ref[at : at + 1, :]
    wide = jnp.concatenate([gram, jnp.zeros((count, LANES - count), jnp.float32)], axis=1)
    if len(outs) > 2:
        share_out, gram_out, _ = outs
        share_out[...] = share
        gram_out[...] = wide
        return
    send_ref, turned_ref = outs
    traces = tile_traces(sizes, tiles)
    own_rows = lambda values: [values[0:8], values[32:40]]
    table = jnp.concatenate(
        [share] + own_rows(traces) + own_rows(jnp.broadcast_to(group.astype(jnp.float32), (count, frames)))
        + [jnp.zeros((LANES - count - 32, frames), jnp.float32)],
        axis=0,
    )
    turned_ref[...] = jnp.transpose(table)
    chunk = [wide[8 * at : 8 * at + 8] for at in range(6)]
    place = lane_iota((8, LANES))
    first = pltpu.roll(chunk[0], 80, axis=1)
    tail = pltpu.roll(chunk[5], 96, axis=1)
    second = chunk[1] + pltpu.roll(chunk[2], 48, axis=1) + jnp.where(place >= 96, tail, 0.0)
    third = chunk[3] + pltpu.roll(chunk[4], 48, axis=1) + pltpu.roll(jnp.where(place < 16, tail, 0.0), 96, axis=1)
    for at in range(devices):
        send_ref[at, 0:8, :] = turned_ref[pl.ds(at, 8, stride=devices), :] + first
        send_ref[at, 8:16, :] = second
        send_ref[at, 16:24, :] = third


def shape_kernel(
    sizes, own_ref, west_ref, north_ref, corner_ref, movie_ref, back_ref, back_trace_ref, window_ref,
    start_ref, code_ref, parts_ref, own_out, west_out, row_out, value_ref, goal_ref, split_ref,
):
    tiles = (own_ref, west_ref, north_ref, corner_ref)
    count = value_ref.shape[0]
    pixels, frames = sizes.pixels, sizes.frames
    part = 512
    group = tile_labels(sizes, tiles)[2]
    traces = tile_traces(sizes, tiles)
    moment = lane_iota((count, frames))
    inside = (moment >= window_ref[0]) & (moment < window_ref[1])
    weighted = jnp.where(inside, traces, 0.0)
    overlap = lax.dot_general(
        weighted, weighted, TRANS_B, precision=lax.Precision.HIGHEST, preferred_element_type=jnp.float32
    )
    mass = jnp.sum(weighted * weighted, axis=1, keepdims=True)
    inverse = 1.0 / jnp.where(group >= 0, mass, 1.0)
    overlap = jnp.where(sub_iota((count, count)) == lane_iota((count, count)), 0.0, overlap * inverse)
    rate = jnp.concatenate([overlap, overlap], axis=1)
    rate_high = rate.astype(jnp.bfloat16)
    rate_low = (rate - rate_high.astype(jnp.float32)).astype(jnp.bfloat16)
    rates = jnp.concatenate([rate_high, rate_low], axis=0)
    loads = [
        jnp.sum(weighted * back_trace_ref[at : at + 1, :], axis=1, keepdims=True) * inverse for at in range(2)
    ]
    rounded = weighted.astype(jnp.bfloat16)
    for at in range(0, pixels, part):
        goal = lax.dot_general(
            rounded, movie_ref[at : at + part, :], TRANS_B, preferred_element_type=jnp.float32
        ) * inverse
        for back in range(2):
            goal = goal - loads[back] * back_ref[back : back + 1, at : at + part].astype(jnp.float32)
        goal_ref[:, at : at + part] = goal
    for step in range(GROUPS):
        values, parts = (start_ref, parts_ref) if step == 0 else (value_ref, split_ref)
        for at in range(0, pixels, part):
            coupled = jnp.dot(rates, parts[0 : 2 * count, at : at + part], preferred_element_type=jnp.float32)
            coupled = coupled[:count] + coupled[count:]
            value = jnp.where(
                code_ref[:, at : at + part] == step,
                jnp.maximum(goal_ref[:, at : at + part] - coupled, 0.0),
                values[:, at : at + part],
            )
            value_ref[:, at : at + part] = value
            if step < GROUPS - 1:
                high = value.astype(jnp.bfloat16)
                split_ref[0:count, at : at + part] = high
                split_ref[count : 2 * count, at : at + part] = (value - high.astype(jnp.float32)).astype(jnp.bfloat16)
    half = pixels // 2
    own_out[:, :pixels] = value_ref[0:8, :]
    west_out[:, :pixels] = value_ref[8:16, :]
    row_out[0:8, :pixels] = value_ref[16:24, :]
    row_out[8:16, :pixels] = value_ref[24:32, :]
    low = sub_iota((SUBLANES, half)) < 4
    for base, even, odd, shift in ((32, own_out, west_out, 0), (40, row_out, row_out, 8)):
        left, right_half = value_ref[base : base + 8, :half], value_ref[base : base + 8, half:]
        even[0:8, pixels:] = jnp.where(low, left, half_swap(right_half))
        odd[shift : shift + 8, pixels:] = jnp.where(low, half_swap(left), right_half)


def trace_kernel(rows, cols, step_frames, recv_ref, out_ref, coupling_ref, near_ref, turned_ref):
    count = 4 * 12
    lane = lane_iota((SUBLANES * 6, LANES))
    west = LANES - step_frames
    low = sub_iota((SUBLANES, LANES)) < 4
    shares, starts, codes, selfs = [], [], [], []
    for r in range(rows):
        tables = [
            jnp.transpose(recv_ref[r * cols : (r + 1) * cols, 8 * at : 8 * at + 8, :].reshape(LANES, LANES))
            for at in range(3)
        ]
        shares.append(tables[0][0:48])
        starts.append((tables[0][48:56], tables[0][56:64]))
        codes.append((tables[0][64:72], tables[0][72:80]))
        chunks = [
            tables[0][80:128], tables[1][0:48], tables[1][48:96], tables[2][0:48], tables[2][48:96],
            jnp.concatenate([tables[1][96:128], tables[2][96:112]], axis=0),
        ]
        pieces = []
        for a, chunk in enumerate(chunks):
            diagonal = jnp.zeros((SUBLANES, LANES), jnp.float32)
            for t in range(SUBLANES):
                spread = jnp.take_along_axis(
                    chunk, (lane // SUBLANES) * SUBLANES + t, axis=1, mode="promise_in_bounds"
                )
                here = sub_iota((SUBLANES, LANES)) == t
                same = spread[8 * a : 8 * a + 8]
                diagonal = diagonal + jnp.where(here, same, 0.0)
                coupling_ref[r, 8 * a + t] = spread
                coupling_ref[r, 8 * a + t, 8 * a : 8 * a + 8] = jnp.where(here, 0.0, same)
            pieces.append(diagonal)
        selfs.append(jnp.concatenate(pieces, axis=0))

    def collect(per_tile, r):
        here = per_tile[r]
        top = here[0:8] + pltpu.roll(here[8:16], west, axis=1)
        rest = here[32:40] + half_swap(pltpu.roll(here[32:40], west, axis=1))
        if r + 1 < rows:
            below = per_tile[r + 1]
            top = top + below[16:24] + pltpu.roll(below[24:32], west, axis=1)
            rest = rest + below[40:48] + half_swap(pltpu.roll(below[40:48], west, axis=1))
        return top, rest

    drive = [collect(shares, r) for r in range(rows)]
    weight = [collect(selfs, r) for r in range(rows)]
    inverse = [
        [1.0 / jnp.where(code >= 0, total, 1.0) for code, total in zip(codes[r], weight[r])] for r in range(rows)
    ]
    current = [list(starts[r]) for r in range(rows)]
    for step in range(GROUPS):
        for r in range(rows):
            top, rest = current[r]
            rest_pair = jnp.where(low, rest, half_swap(pltpu.roll(rest, step_frames, axis=1)))
            near_ref[r, 0:8] = top
            near_ref[r, 8:16] = pltpu.roll(top, step_frames, axis=1)
            near_ref[r, 32:40] = rest_pair
            if r + 1 < rows:
                near_ref[r + 1, 16:24] = top
                near_ref[r + 1, 24:32] = pltpu.roll(top, step_frames, axis=1)
                near_ref[r + 1, 40:48] = rest_pair
            if r == 0:
                near_ref[r, 16:32] = jnp.zeros((16, LANES), jnp.float32)
                near_ref[r, 40:48] = jnp.zeros((8, LANES), jnp.float32)
        sums = []
        for r in range(rows):
            total = jnp.zeros((count, LANES), jnp.float32)
            for k in range(count):
                total = total + coupling_ref[r, k] * near_ref[r, k : k + 1, :]
            sums.append(total)
        for r in range(rows):
            for at, coupled in enumerate(collect(sums, r)):
                updated = jnp.maximum((drive[r][at] - coupled) * inverse[r][at], 0.0)
                current[r][at] = jnp.where(codes[r][at] == step, updated, current[r][at])
    for r in range(rows):
        table = jnp.concatenate(
            [current[r][0], jnp.where(low, current[r][1], 0.0), jnp.zeros((LANES - 16, LANES), jnp.float32)], axis=0
        )
        turned_ref[...] = jnp.transpose(table)
        out = jnp.zeros((cols, LANES), jnp.float32)
        for t in range(step_frames):
            out = out + pltpu.roll(turned_ref[pl.ds(t, cols, stride=step_frames), :], 16 * t, axis=1)
        out_ref[r * cols : (r + 1) * cols, :] = out


def finish_kernel(sizes, side, slices, own_ref, row_ref, east_ref, anchor_ref, *refs):
    slots = anchor_ref.shape[1]
    pixels, half = sizes.pixels, sizes.pixels // 2
    count = pixels // LANES
    new_footprint_ref = refs[-2] if slices else refs[-1]
    back_down = (side - column_of(anchor_ref[0:1, :], slots)) % side
    back_right = (side - column_of(anchor_ref[1:2, :], slots)) % side
    strips = []
    for at in range(0, pixels, LANES):
        where_rest = pixels + at % half
        top = own_ref[:, at : at + LANES] + row_ref[0:8, at : at + LANES] + east_ref[:, at : at + LANES]
        rest = (
            own_ref[:, where_rest : where_rest + LANES]
            + row_ref[0:8, where_rest : where_rest + LANES]
            + east_ref[:, where_rest : where_rest + LANES]
        )
        if at >= half:
            rest = half_swap(rest)
        strips.append(jnp.concatenate([top, rest[: slots - SUBLANES]], axis=0))
    strips = rolled(strips, back_down, back_right, side)
    for at, strip in enumerate(strips):
        new_footprint_ref[pl.ds(at, slots, stride=count), :] = strip
    if not slices:
        return
    recv_ref, _, new_trace_ref = refs
    table = jnp.transpose(
        jnp.concatenate([recv_ref[...], jnp.zeros((LANES - slices, LANES), jnp.float32)], axis=0)
    )
    per = LANES // slices
    count = sizes.frames // LANES
    for tile in range(count):
        out = jnp.zeros((16, LANES), jnp.float32)
        for at in range(per):
            t = tile * per + at
            out = out + pltpu.roll(table[16 * t : 16 * t + 16], slices * at, axis=1)
        new_trace_ref[pl.ds(tile, slots, stride=count), :] = out[:slots]


def padded(cells, sides):
    for axis, dim in sides:
        size = cells.shape[dim]
        head = lax.slice_in_dim(cells, 0, 1, axis=dim)
        tail = lax.slice_in_dim(cells, size - 1, size, axis=dim)
        cells = jnp.concatenate([shifted(tail, axis, 1), cells, shifted(head, axis, -1)], axis=dim)
    return cells


def relax_by_neighbours(share, gram, traces, group, alive):
    slots, frames = traces.shape
    rows_of = lambda values: [
        jnp.concatenate([values[8 * b : 8 * b + 8], values[32 + 4 * b : 36 + 4 * b]], axis=0) for b in range(4)
    ]
    shares = rows_of(share)
    grams = [rows_of(part.T) for part in rows_of(gram)]
    near = []
    for b in range(4):
        cells = [[jnp.zeros((slots, slots), jnp.float32)] * 3 for _ in range(3)]
        for k in range(4):
            cells[1 + b // 2 - k // 2][1 + b % 2 - k % 2] = grams[b][k].T
        near.append(jnp.concatenate([cell for row in cells for cell in row], axis=1))
    both = jnp.stack([jnp.concatenate(pair, axis=1) for pair in zip(shares, near)]).reshape(2, 2, slots, -1)
    column_sum = both[:, 0] + shifted(both[:, 1], "col", -1)
    total = column_sum[0] + shifted(column_sum[1], "row", -1)
    drives, coupling = total[:, :frames], total[:, frames:]
    weight = jnp.diagonal(coupling[:, 4 * slots : 5 * slots])
    weight = jnp.where(alive, weight, 1.0)
    for step in range(GROUPS):
        nearby = padded(traces[None, None], (("row", 0), ("col", 1))).reshape(9 * slots, frames)
        coupled = jnp.dot(coupling, nearby, precision=lax.Precision.HIGHEST)
        updated = jnp.maximum(traces + (drives - coupled) / weight[:, None], 0.0)
        traces = jnp.where((alive & (group == step))[:, None], updated, traces)
    return traces


def shifted(value, axis, steps):
    count = lax.axis_size(axis)
    initial, last = (max(0, -steps), min(count, count - steps))
    return lax.ppermute(value, axis, [(source, source + steps) for source in range(initial, last)])


VMEM = pl.BlockSpec(memory_space=pltpu.VMEM)
SMEM = pl.BlockSpec(memory_space=pltpu.SMEM)


def kernel_params(megabytes):
    return pltpu.CompilerParams(vmem_limit_bytes=megabytes * 2**20)


def on_device(rows, cols, movie, footprints, anchors, groups, counts, temporal, back_spatial, back_temporal, window):
    tile_rows, tile_cols, frames = movie.shape
    slots = footprints.shape[2]
    pixels = tile_rows * tile_cols
    side = tile_cols
    assert pixels == footprints.shape[3] and tile_rows == side and 2 * side == LANES and slots == 12
    devices = rows * cols
    step_frames = frames // devices
    sliced = step_frames * devices == frames and step_frames == SUBLANES and cols * step_frames == LANES
    count = 4 * slots
    sizes = Sizes(pixels, frames)
    anchor = anchors[0, 0].T
    f32 = lambda *shape: jax.ShapeDtypeStruct(shape, jnp.float32)
    packed = pl.pallas_call(
        functools.partial(pack_kernel, sizes, side),
        out_shape=f32(SUBLANES, sizes.packed),
        in_specs=[VMEM, VMEM, VMEM, SMEM, VMEM],
        out_specs=VMEM,
        compiler_params=kernel_params(3),
        name="pack",
    )(footprints.reshape(-1, LANES), anchor, groups[0], counts, temporal.reshape(-1, LANES))
    north = shifted(packed, "row", 1)
    west = shifted(packed, "col", 1)
    corner = shifted(west, "row", 1)
    near_movie = pl.pallas_call(
        movie_kernel,
        out_shape=jax.ShapeDtypeStruct((pixels, frames), movie.dtype),
        in_specs=[pl.BlockSpec(memory_space=pl.ANY)] * 2,
        out_specs=VMEM,
        scratch_shapes=[pltpu.SemaphoreType.DMA(())],
        compiler_params=kernel_params(3),
        cost_estimate=pl.CostEstimate(flops=10**7, bytes_accessed=pixels * frames * 4, transcendentals=0),
        name="stage",
    )(packed, movie.reshape(pixels, frames))
    back = jnp.pad(back_spatial.reshape(2, pixels), ((0, 14), (0, 0)))
    if sliced:
        share_outs, share_scratch = (f32(devices, 24, LANES),), [pltpu.VMEM((frames, LANES), jnp.float32)]
    else:
        share_outs = (f32(count, frames), f32(count, LANES))
        share_scratch = [pltpu.VMEM((SUBLANES, LANES), jnp.float32)]
    canvas, code, split, *shares = pl.pallas_call(
        functools.partial(share_kernel, sizes, side, devices),
        out_shape=(
            f32(count, pixels),
            jax.ShapeDtypeStruct((count, pixels), jnp.int32),
            jax.ShapeDtypeStruct((2 * count + 16, pixels), jnp.bfloat16),
        )
        + share_outs,
        in_specs=[VMEM] * 7,
        out_specs=(VMEM,) * (3 + len(share_outs)),
        scratch_shapes=share_scratch,
        compiler_params=kernel_params(10),
        cost_estimate=pl.CostEstimate(flops=10**9, bytes_accessed=8 * 2**20, transcendentals=0),
        name="share",
    )(packed, west, north, corner, near_movie, back, back_temporal)
    own_part, west_part, row_part = pl.pallas_call(
        functools.partial(shape_kernel, sizes),
        out_shape=(f32(SUBLANES, sizes.trace), f32(SUBLANES, sizes.trace), f32(2 * SUBLANES, sizes.trace)),
        in_specs=[VMEM] * 7 + [SMEM] + [VMEM] * 3,
        out_specs=(VMEM,) * 3,
        scratch_shapes=[
            pltpu.VMEM((count, pixels), jnp.float32),
            pltpu.VMEM((count, pixels), jnp.float32),
            pltpu.VMEM((2 * count, pixels), jnp.bfloat16),
        ],
        compiler_params=kernel_params(12),
        cost_estimate=pl.CostEstimate(flops=10**9, bytes_accessed=8 * 2**20, transcendentals=0),
        name="shape",
    )(packed, west, north, corner, near_movie, back, back_temporal, window, canvas, code, split)
    from_south = shifted(row_part, "row", -1)
    from_east = shifted(west_part + from_south[SUBLANES:], "col", -1)
    if sliced:
        received = lax.all_to_all(shares[0], ("row", "col"), 0, 0, tiled=True)
        relaxed = pl.pallas_call(
            functools.partial(trace_kernel, rows, cols, step_frames),
            out_shape=f32(devices, LANES),
            in_specs=[VMEM],
            out_specs=VMEM,
            scratch_shapes=[
                pltpu.VMEM((rows, count, count, LANES), jnp.float32),
                pltpu.VMEM((rows, count, LANES), jnp.float32),
                pltpu.VMEM((LANES, LANES), jnp.float32),
            ],
            compiler_params=kernel_params(6),
            cost_estimate=pl.CostEstimate(flops=10**9, bytes_accessed=2**20, transcendentals=0),
            name="relax",
        )(received)
        extra = (lax.all_to_all(relaxed, ("row", "col"), 0, 0, tiled=True),)
    else:
        alive = jnp.arange(slots, dtype=jnp.int32) < counts[0, 0]
        traces = relax_by_neighbours(shares[0], shares[1][:, :count], temporal[0, 0], groups[0, 0], alive)
        extra = ()
    new_footprints, *new_traces = pl.pallas_call(
        functools.partial(finish_kernel, sizes, side, devices if sliced else 0),
        out_shape=(f32(slots * pixels // LANES, LANES),) + (f32(slots * frames // LANES, LANES),) * len(extra),
        in_specs=[VMEM] * (4 + len(extra)),
        out_specs=(VMEM,) * (1 + len(extra)),
        compiler_params=kernel_params(4),
        name="finish",
    )(own_part, from_south, from_east, anchor, *extra)
    if sliced:
        traces = new_traces[0]
    return new_footprints.reshape(footprints.shape), traces.reshape(temporal.shape)


def solution(mesh):
    return jax.shard_map(
        functools.partial(on_device, mesh.shape["row"], mesh.shape["col"]),
        mesh=mesh,
        in_specs=(
            P("row", "col", None),
            P("row", "col", None, None),
            P("row", "col", None, None),
            P("row", "col", None),
            P("row", "col"),
            P("row", "col", None, None),
            P(None, "row", "col"),
            P(),
            P(),
        ),
        out_specs=(P("row", "col", None, None), P("row", "col", None, None)),
        check_vma=False,
    )
```
